32 devices in a mesh: wide: 4 (over y, x), narrow: 8 (over z, core).
Axes of the slice: x: 2, y: 2, z: 4, core: 2. Of those that a mesh axis runs over, the one named last changes fastest.
Arguments:
- charges: bfloat16 [512, 256, 128], P(('wide', 'narrow')), may hold values from -6 to 6
- pairs_first: int32 [2048, 4], P(('wide', 'narrow')), may hold values from 0 to 15, as said below
- pairs_second: int32 [2048, 4], P(('wide', 'narrow')), may hold values from 0 to 15, as said below
- pairs_third: int32 [2048, 4], P(('wide', 'narrow')), may hold values from 0 to 15, as said below
- matrices_first: bfloat16 [256, 256, 256], P(('wide', 'narrow')), may hold values from -0.21875 to 0.21875
- matrices_second: bfloat16 [256, 256, 256], P(('wide', 'narrow')), may hold values from -0.21875 to 0.21875
- matrices_third: bfloat16 [256, 256, 256], P(('wide', 'narrow')), may hold values from -0.21875 to 0.21875
- box_owner: int32 [4, 8, 16], P('wide', 'narrow'), may hold values from 0 to 3, as said below
Outputs:
- potentials: bfloat16 [512, 256, 128], P(('wide', 'narrow'))
The draws below stay inside these ranges and needn't reach their ends.
Inputs may be any that keep to these rules, and one draw needn't show every extreme that they name: `pairs_first`: each device's 64 rows hold a source box and a target box below 16, a matrix below 8 and a live flag 0 or 1; live rows come before the others; in every list some device has all rows live. `pairs_second`: same form as pairs_first. `pairs_third`: same form as pairs_first. `box_owner`: for each narrow index, every wide index hands 0 or 8 of its boxes to each owner, and each owner receives exactly 16 boxes.
All inputs are finite; a program needn't handle non-finite values.
Results may differ from the reference program's by a relative error of at most 0.0057.
Values may be sent and summed in bfloat16 or wider, within the bound.
No kernel may reach another device: no remote copies, remote signals or barrier semaphores. Data moves between devices by JAX's collectives and lax.ppermute only.
A program may use at most 64 MiB of HBM per device.

```python
import jax
import jax.numpy as jnp
from jax import lax

R = 256
RHS = 128
BOX_DEV = 16
PAIRS = 64
TRANS_DEV = 8
CAP = 8
HOLD = 16
BOXES = 512
N_WIDE = 4
N_NARROW = 8
DEVICES = 32


def pair_lists(key, salt):
    key = jax.random.fold_in(key, salt)
    keys = jax.random.split(key, 5)
    device_count = N_WIDE * N_NARROW
    sources = jax.random.randint(keys[0], (device_count, PAIRS), 0, BOX_DEV)
    targets = jax.random.randint(keys[1], (device_count, PAIRS), 0, BOX_DEV)
    tables = jax.random.randint(keys[2], (device_count, PAIRS), 0, TRANS_DEV)
    lengths = jax.random.randint(keys[3], (device_count, 1), 2, PAIRS + 1)
    longest = jax.random.randint(keys[4], (), 0, device_count)
    devices = jnp.arange(device_count, dtype=jnp.int32)[:, None]
    lengths = jnp.where(devices == longest, PAIRS, lengths)
    live = (jnp.arange(PAIRS, dtype=jnp.int32)[None, :] < lengths).astype(jnp.int32)
    stacked = jnp.stack([sources, targets, tables, live], axis=-1)
    return stacked.reshape(device_count * PAIRS, 4).astype(jnp.int32)


def draw_pairs_first(key, part):
    return pair_lists(key, 11)


def draw_pairs_second(key, part):
    return pair_lists(key, 23)


def draw_pairs_third(key, part):
    return pair_lists(key, 37)


def draw_box_owner(key, part):
    half = N_WIDE // 2

    def column(narrow_pos):
        column_key = jax.random.fold_in(key, narrow_pos)

        def couple(couple_pos):
            couple_key = jax.random.fold_in(column_key, couple_pos)
            keys = jax.random.split(couple_key, 3)
            order = jax.random.permutation(keys[0], N_WIDE).astype(jnp.int32)
            lower = jnp.repeat(order[:half], CAP)
            upper = jnp.repeat(order[half:], CAP)
            lower = jax.random.permutation(keys[1], lower)
            upper = jax.random.permutation(keys[2], upper)
            return jnp.stack([lower, upper], axis=0)
        rows = jax.vmap(couple)(jnp.arange(half, dtype=jnp.int32))
        return rows.reshape(N_WIDE, BOX_DEV)
    columns = jax.vmap(column)(jnp.arange(N_NARROW, dtype=jnp.int32))
    return jnp.transpose(columns, (1, 0, 2)).astype(jnp.int32)


def block_scale(stream_key, shape, cuts, low, top_value):
    def one(axis_at, parts):
        steps = jax.random.uniform(jax.random.fold_in(jax.random.fold_in(stream_key, 6), axis_at), (parts,), jnp.float32, low / len(cuts), top_value / len(cuts))
        return jnp.repeat(jnp.exp(steps), shape[axis_at] // parts).reshape((-1,) + (1,) * (len(shape) - axis_at - 1))

    level = one(*cuts[0])
    for cut in cuts[1:]:
        level = level * one(*cut)
    return level


def normal_values(stream_key, extent, deviation, most, shards=(), kind=jnp.bfloat16):
    array = deviation * jax.random.normal(stream_key, extent, jnp.float32)
    if shards:
        array = array * block_scale(stream_key, extent, shards, -0.22, 0.18)
    return jnp.clip(array, -most, most).astype(kind)


def setup_inputs(seed: int = 0) -> dict:
    key_of = jax.random.split(jax.random.key(seed), 9)
    return {
        "charges": normal_values(key_of[0], (BOXES, R, RHS), 1.0, 6.0, ((0, 32),)),
        "pairs_first": draw_pairs_first(jax.random.fold_in(key_of[8], 71), 0),
        "pairs_second": draw_pairs_second(jax.random.fold_in(key_of[8], 71), 0),
        "pairs_third": draw_pairs_third(jax.random.fold_in(key_of[8], 71), 0),
        "matrices_first": normal_values(key_of[4], (DEVICES * TRANS_DEV, R, R), (3 * R) ** -0.5, 0.21875, ((0, 32),)),
        "matrices_second": normal_values(key_of[5], (DEVICES * TRANS_DEV, R, R), (3 * R) ** -0.5, 0.21875, ((0, 32),)),
        "matrices_third": normal_values(key_of[6], (DEVICES * TRANS_DEV, R, R), (3 * R) ** -0.5, 0.21875, ((0, 32),)),
        "box_owner": draw_box_owner(jax.random.fold_in(key_of[8], 71), 0),
    }


def translate(coeffs, pairs, mats):
    device_count = coeffs.shape[0] // BOX_DEV
    blocks = coeffs.reshape(device_count, BOX_DEV, R, RHS)
    lists = pairs.reshape(device_count, PAIRS, 4)
    tables = mats.reshape(device_count, TRANS_DEV, R, R)

    def device_level(packed):
        block, listing, table = packed

        def add_pair(running, pair_row):
            matrix = lax.dynamic_index_in_dim(table, pair_row[2], 0, keepdims=False)
            source = lax.dynamic_index_in_dim(block, pair_row[0], 0, keepdims=False)
            product = jnp.dot(matrix, source, preferred_element_type=jnp.float32)
            weight = pair_row[3].astype(jnp.float32)
            return running.at[pair_row[1]].add(weight * product), jnp.zeros((), jnp.float32)

        running, unused = lax.scan(add_pair, jnp.zeros((BOX_DEV, R, RHS), jnp.float32), listing)
        return running.astype(jnp.bfloat16)

    return lax.map(device_level, (blocks, lists, tables)).reshape(coeffs.shape)


def regroup_narrow(coeffs):
    grid = coeffs.reshape(N_WIDE, N_NARROW, BOX_DEV, N_NARROW, R // N_NARROW, RHS)
    grid = jnp.transpose(grid, (0, 3, 2, 1, 4, 5))
    return grid.reshape(coeffs.shape)


def regroup_wide(coeffs):
    grid = coeffs.reshape(N_WIDE, N_NARROW, BOX_DEV, N_WIDE, R // N_WIDE, RHS)
    grid = jnp.transpose(grid, (3, 1, 2, 0, 4, 5))
    return grid.reshape(coeffs.shape)


def handover(final, box_owner):
    grid = final.reshape(N_WIDE, N_NARROW, BOX_DEV, R * RHS)
    flat_count = N_WIDE * BOX_DEV

    def column(narrow_pos):
        boxes = grid[:, narrow_pos].reshape(flat_count, R * RHS)
        owners = box_owner[:, narrow_pos].reshape(flat_count)
        hit = (owners[None, :] == jnp.arange(N_WIDE, dtype=jnp.int32)[:, None]).astype(jnp.int32)
        placed = jnp.cumsum(hit, axis=1) - hit
        slots = jnp.arange(HOLD, dtype=jnp.int32)
        select = hit[:, None, :] * (placed[:, None, :] == slots[None, :, None]).astype(jnp.int32)
        select = select.reshape(N_WIDE * HOLD, flat_count).astype(jnp.bfloat16)
        return jnp.dot(select, boxes, preferred_element_type=jnp.float32).astype(jnp.bfloat16)

    result = lax.map(column, jnp.arange(N_NARROW, dtype=jnp.int32))
    result = result.reshape(N_NARROW, N_WIDE, HOLD, R, RHS)
    result = jnp.transpose(result, (1, 0, 2, 3, 4))
    return result.reshape(N_WIDE * N_NARROW * HOLD, R, RHS)


def reference(charges, pairs_first, pairs_second, pairs_third, matrices_first, matrices_second, matrices_third, box_owner):
    first = translate(charges, pairs_first, matrices_first)
    second = translate(regroup_narrow(first), pairs_second, matrices_second)
    final = translate(regroup_wide(second), pairs_third, matrices_third)
    return handover(final, box_owner)
```

```python
import functools

import jax
import jax.numpy as jnp
from jax import lax
from jax.experimental import pallas as pl
from jax.experimental.pallas import tpu as pltpu
from jax.sharding import PartitionSpec as P


UNROLL = 4
VMEM = pl.BlockSpec(memory_space=pltpu.VMEM)
SMEM = pl.BlockSpec(memory_space=pltpu.SMEM)


def partners(size):
    top = size // 2
    far = [r for r in range(1, size) if r >= top]
    near = [r for r in range(1, size) if r < top]
    return far + sorted(near, key=lambda r: (r < 2, r))


def left_half(shape):
    return lax.broadcasted_iota(jnp.int32, shape, len(shape) - 1) < shape[-1] // 2


def swap(block):
    return pltpu.roll(block, block.shape[-1] // 2, block.ndim - 1)


def live_count(pairs):
    count = pairs[0, 3]
    for row in range(1, pairs.shape[0]):
        count = count + pairs[row, 3]
    return count


def accumulate(pairs, mats, source, place, acc):
    dummy = acc.shape[0] - 1

    def group(index, carry):
        products = []
        for step in range(UNROLL):
            row = index * UNROLL + step
            slot, half = place(pairs[row, 1])
            slot = jnp.where(pairs[row, 3] > 0, slot, dummy)
            product = jnp.dot(
                mats[pairs[row, 2]], source(pairs[row, 0], half),
                preferred_element_type=jnp.float32,
            )
            products.append((slot, product))
        for slot, product in products:
            acc[slot] += product
        return carry

    lax.fori_loop(0, (live_count(pairs) + UNROLL - 1) // UNROLL, group, 0)


def clear(acc):
    def one(index, carry):
        acc[index] = jnp.zeros(acc.shape[1:], acc.dtype)
        return carry

    lax.fori_loop(0, acc.shape[0], one, 0)


def first_kernel(size, me_ref, pairs, charges, mats, *refs):
    outs, acc = refs[:-1], refs[-1]
    me = me_ref[0]
    boxes, width, columns = charges.shape
    piece = width // size
    clear(acc)
    accumulate(
        pairs, mats, lambda s, half: charges[s], lambda k: (k, 0), acc
    )
    left = left_half((piece, columns))
    for r in range(size):
        rows = pl.ds(pl.multiple_of((me ^ r) * piece, piece), piece)

        def one(i, carry, r=r, rows=rows):
            a = acc[2 * i, rows, :]
            b = acc[2 * i + 1, rows, :]
            outs[r][i] = jnp.where(left, a, swap(b)).astype(jnp.bfloat16)
            outs[size + r][i] = jnp.where(left, swap(a), b).astype(jnp.bfloat16)
            return carry

        lax.fori_loop(0, boxes // 2, one, 0, unroll=True)


def assemble(me, ins, view):
    count, piece, columns = ins[0].shape
    left = left_half((piece, columns))
    nothing = jnp.zeros((piece, columns), jnp.bfloat16)
    for r, ref in enumerate(ins):
        rows = pl.ds(pl.multiple_of((me ^ r) * piece, piece), piece)
        for i in range(count):
            block = ref[i]
            turned = swap(block)
            view[4 * i, rows, :] = jnp.where(left, block, nothing)
            view[4 * i + 1, rows, :] = jnp.where(left, nothing, turned)
            view[4 * i + 2, rows, :] = jnp.where(left, turned, nothing)
            view[4 * i + 3, rows, :] = jnp.where(left, nothing, block)


def second_kernel(narrow, wide, me_ref, pairs, mats, *refs):
    ins, outs = refs[:narrow], refs[narrow : narrow + wide]
    acc, view = refs[narrow + wide :]
    count, piece, columns = outs[0].shape
    assemble(me_ref[0], ins, view)
    clear(acc)
    accumulate(
        pairs, mats, lambda s, half: view[2 * s + half],
        lambda k: (k >> 1, k & 1), acc,
    )
    for r in range(wide):
        rows = pl.ds(pl.multiple_of((me_ref[1] ^ r) * piece, piece), piece)
        for i in range(count):
            outs[r][i] = acc[i, rows, :].astype(jnp.bfloat16)


def third_kernel(wide, me_ref, owners, pairs, mats, *refs):
    ins, outs = refs[:wide], refs[wide : 2 * wide]
    acc, view, filled, spots = refs[2 * wide :]
    boxes = owners.shape[0]
    width, columns = acc.shape[1:]
    room = 2 * boxes // wide
    for o in range(wide):
        filled[o] = 0
    for k in range(boxes):
        o = owners[k]
        spots[k] = o * room + filled[o]
        filled[o] = filled[o] + 1
    assemble(me_ref[1], ins, view)
    clear(acc)
    accumulate(
        pairs, mats, lambda s, half: view[2 * s + half],
        lambda k: (spots[k] >> 1, spots[k] & 1), acc,
    )
    for r in range(wide):
        o = me_ref[1] ^ r
        flag = (filled[o] > 0).astype(jnp.float32)
        for p in range(room // 2):
            outs[r][pl.ds(p * width, width), :] = acc[o * (room // 2) + p].astype(jnp.bfloat16)
        tail = outs[r].shape[0] - room // 2 * width
        outs[r][pl.ds(room // 2 * width, tail), :] = jnp.full(
            (tail, columns), flag, jnp.float32
        ).astype(jnp.bfloat16)


def last_kernel(wide, me_ref, *refs):
    ins, out, flags = refs[: 2 * wide], refs[2 * wide], refs[2 * wide + 1]
    boxes, width, columns = out.shape
    room = 2 * boxes // wide
    me = me_ref[1]
    for r in range(wide):
        mark = ins[r][pl.ds(room // 2 * width, 16), :].astype(jnp.float32)
        flags[me ^ r] = (jnp.max(mark) > 0.5).astype(jnp.int32)
    left = left_half((width, columns))
    for r in range(wide):
        origin = me ^ r
        base = jnp.int32(0)
        for w in range(wide):
            base = base + jnp.where(w < origin, flags[w], 0) * room

        @pl.when(flags[origin] > 0)
        def _(r=r, base=base):
            for p in range(room // 2):
                a = ins[r][pl.ds(p * width, width), :]
                b = ins[wide + r][pl.ds(p * width, width), :]
                out[base + 2 * p] = jnp.where(left, a, swap(b))
                out[base + 2 * p + 1] = jnp.where(left, swap(a), b)


def exchange(parts, axis, size):
    moved = [parts[0]] + [None] * (size - 1)
    for r in partners(size):
        moved[r] = lax.ppermute(parts[r], axis, [(i, i ^ r) for i in range(size)])
    return moved


def cost(pair_count, width, columns, moved):
    return pl.CostEstimate(
        flops=2 * pair_count * width * width * columns, bytes_accessed=moved, transcendentals=0
    )


def per_device(
    narrow, wide, charges, pairs_first, pairs_second, pairs_third,
    matrices_first, matrices_second, matrices_third, box_owner,
):
    boxes, width, columns = charges.shape
    pair_count = pairs_first.shape[0]
    half = boxes // 2
    room = 2 * boxes // wide
    me = jnp.stack([lax.axis_index("narrow"), lax.axis_index("wide")]).astype(jnp.int32)
    owners = box_owner.reshape(boxes)
    estimate = cost(pair_count, width, columns, 4 * boxes * width * columns)

    def blocks(shape, count):
        return [jax.ShapeDtypeStruct(shape, jnp.bfloat16)] * count

    sent = pl.pallas_call(
        functools.partial(first_kernel, narrow),
        out_shape=blocks((half, width // narrow, columns), 2 * narrow),
        in_specs=[SMEM, SMEM, VMEM, VMEM],
        out_specs=[VMEM] * (2 * narrow),
        scratch_shapes=[pltpu.VMEM((boxes + 1, width, columns), jnp.float32)],
        cost_estimate=estimate,
        name="first_level",
    )(me, pairs_first, charges, matrices_first)

    view = pltpu.VMEM((2 * boxes, width, columns), jnp.bfloat16)
    second = pl.pallas_call(
        functools.partial(second_kernel, narrow, wide),
        out_shape=blocks((half, width // wide, columns), wide),
        in_specs=[SMEM, SMEM, VMEM] + [VMEM] * narrow,
        out_specs=[VMEM] * wide,
        scratch_shapes=[pltpu.VMEM((half + 1, width, columns), jnp.float32), view],
        cost_estimate=estimate,
        name="second_level",
    )
    third = pl.pallas_call(
        functools.partial(third_kernel, wide),
        out_shape=blocks((room // 2 * width + 16, columns), wide),
        in_specs=[SMEM, SMEM, SMEM, VMEM] + [VMEM] * wide,
        out_specs=[VMEM] * wide,
        scratch_shapes=[
            pltpu.VMEM((wide * room // 2 + 1, width, columns), jnp.float32), view,
            pltpu.SMEM((wide,), jnp.int32), pltpu.SMEM((boxes,), jnp.int32),
        ],
        cost_estimate=estimate,
        name="third_level",
    )
    moved = [exchange(sent[c * narrow : (c + 1) * narrow], "narrow", narrow) for c in range(2)]
    moved = [exchange(second(me, pairs_second, matrices_second, *m), "wide", wide) for m in moved]
    moved = [exchange(third(me, owners, pairs_third, matrices_third, *m), "wide", wide) for m in moved]
    return pl.pallas_call(
        functools.partial(last_kernel, wide),
        out_shape=jax.ShapeDtypeStruct((boxes, width, columns), jnp.bfloat16),
        in_specs=[SMEM] + [VMEM] * (2 * wide),
        out_specs=VMEM,
        scratch_shapes=[pltpu.SMEM((wide,), jnp.int32)],
        name="place",
    )(me, *moved[0], *moved[1])


def solution(mesh):
    rows = P(("wide", "narrow"), None)
    blocks = P(("wide", "narrow"), None, None)
    return jax.shard_map(
        functools.partial(per_device, mesh.shape["narrow"], mesh.shape["wide"]),
        mesh=mesh,
        in_specs=(blocks, rows, rows, rows, blocks, blocks, blocks, P("wide", "narrow", None)),
        out_specs=blocks,
        check_vma=False,
    )
```

```python
import functools

import jax
import jax.numpy as jnp
from jax import lax
from jax.experimental import pallas as pl
from jax.experimental.pallas import tpu as pltpu
from jax.sharding import PartitionSpec as P


UNROLL = 16
PARTS = 4
GRANT = pltpu.CompilerParams(vmem_limit_bytes=16 * 2**20)
VMEM = pl.BlockSpec(memory_space=pltpu.VMEM)
SMEM = pl.BlockSpec(memory_space=pltpu.SMEM)
HBM = pl.BlockSpec(memory_space=pltpu.HBM)


def steps(size):
    top = size // 2
    far, near = list(range(top, size)), list(range(2, top))
    return far[: top // 2] + near + far[top // 2 :] + list(range(1, min(2, top))) + [0]


def left_half(shape):
    return lax.broadcasted_iota(jnp.int32, shape, len(shape) - 1) < shape[-1] // 2


def swap(block):
    return pltpu.roll(block, block.shape[-1] // 2, block.ndim - 1)


def live_count(pairs):
    count = pairs[3, 0]
    for row in range(1, pairs.shape[1]):
        count = count + pairs[3, row]
    return count


def accumulate(pairs, mats, source, place, acc):
    dummy = acc.shape[0] - 1

    def group(index, carry):
        products = []
        for step in range(UNROLL):
            row = index * UNROLL + step
            slot, half = place(pairs[1, row])
            slot = jnp.where(pairs[3, row] > 0, slot, dummy)
            product = jnp.dot(
                mats[pairs[2, row]], source(pairs[0, row], half),
                preferred_element_type=jnp.float32,
            )
            products.append((slot, product))
        for slot, product in products:
            acc[slot] += product
        return carry

    lax.fori_loop(0, (live_count(pairs) + UNROLL - 1) // UNROLL, group, 0)


def clear(acc):
    def one(index, carry):
        acc[index] = jnp.zeros(acc.shape[1:], acc.dtype)
        return carry

    lax.fori_loop(0, acc.shape[0], one, 0)


def fetch(source, target, sems, parts):
    size = source.shape[0] // parts
    copies = [
        pltpu.make_async_copy(
            source.at[pl.ds(p * size, size)], target.at[pl.ds(p * size, size)], sems.at[p]
        )
        for p in range(parts)
    ]
    for copy in copies:
        copy.start()

    def wait():
        for copy in copies:
            copy.wait()

    return wait


def first_kernel(size, pairs_hbm, charges_hbm, mats_hbm, *refs):
    count = 2 * size - 2
    outs, (acc, pairs, charges, mats, sems) = refs[:count], refs[count:]
    waits = [
        fetch(pairs_hbm, pairs, sems.at[0], 1),
        fetch(charges_hbm, charges, sems.at[1], PARTS),
        fetch(mats_hbm, mats, sems.at[2], PARTS),
    ]
    me = lax.axis_index("narrow")
    boxes, width, columns = charges.shape
    piece = width // size
    clear(acc)
    for wait in waits:
        wait()
    accumulate(
        pairs, mats, lambda s, half: charges[s], lambda k: (k, 0), acc
    )
    left = left_half((piece, columns))
    half, far = boxes // 2, size - 2
    for at, r in enumerate(steps(size)):
        rows = pl.ds(pl.multiple_of((me ^ r) * piece, piece), piece)
        targets = (outs[at], outs[far + at]) if at < far else (
            outs[far + at].at[pl.ds(0, half)], outs[far + at].at[pl.ds(half, half)]
        )

        def one(i, carry, targets=targets, rows=rows):
            a = acc[2 * i, rows, :]
            b = acc[2 * i + 1, rows, :]
            targets[0][i] = jnp.where(left, a, swap(b)).astype(jnp.bfloat16)
            targets[1][i] = jnp.where(left, swap(a), b).astype(jnp.bfloat16)
            return carry

        lax.fori_loop(0, half, one, 0, unroll=True)


def assemble(me, ins, view):
    count, piece, columns = ins[0].shape
    left = left_half((piece, columns))
    nothing = jnp.zeros((piece, columns), jnp.bfloat16)
    for r, ref in zip(steps(len(ins)), ins):
        rows = pl.ds(pl.multiple_of((me ^ r) * piece, piece), piece)
        for i in range(count):
            block = ref[i]
            turned = swap(block)
            view[4 * i, rows, :] = jnp.where(left, block, nothing)
            view[4 * i + 1, rows, :] = jnp.where(left, nothing, turned)
            view[4 * i + 2, rows, :] = jnp.where(left, turned, nothing)
            view[4 * i + 3, rows, :] = jnp.where(left, nothing, block)


def second_kernel(narrow, wide, chunk, pairs_hbm, mats, *refs):
    ins, outs = refs[:narrow], refs[narrow : narrow + wide]
    count = outs[0].shape[0]
    ins = [*ins[:-2], *(near.at[pl.ds(chunk * count, count)] for near in ins[-2:])]
    acc, view, pairs, sems = refs[narrow + wide :]
    wait = fetch(pairs_hbm, pairs, sems.at[0], 1)
    me = lax.axis_index("wide")
    count, piece, _ = outs[0].shape
    assemble(lax.axis_index("narrow"), ins, view)
    clear(acc)
    wait()
    accumulate(
        pairs, mats, lambda s, half: view[2 * s + half],
        lambda k: (k >> 1, k & 1), acc,
    )
    for at, r in enumerate(steps(wide)):
        rows = pl.ds(pl.multiple_of((me ^ r) * piece, piece), piece)
        for i in range(count):
            outs[at][i] = acc[i, rows, :].astype(jnp.bfloat16)


def third_kernel(wide, owners_hbm, pairs_hbm, mats, *refs):
    ins, outs = refs[:wide], refs[wide : 2 * wide]
    acc, view, filled, spots, owners, pairs, sems = refs[2 * wide :]
    wait = fetch(pairs_hbm, pairs, sems.at[0], 1)
    wait_owners = fetch(owners_hbm, owners, sems.at[1], 1)
    boxes = owners.shape[1]
    width, columns = acc.shape[1:]
    room = 2 * boxes // wide
    me = lax.axis_index("wide")
    assemble(me, ins, view)
    clear(acc)
    wait_owners()
    for o in range(wide):
        filled[o] = 0
    for k in range(boxes):
        o = owners[0, k]
        spots[k] = o * room + filled[o]
        filled[o] = filled[o] + 1
    wait()
    accumulate(
        pairs, mats, lambda s, half: view[2 * s + half],
        lambda k: (spots[k] >> 1, spots[k] & 1), acc,
    )
    for at, r in enumerate(steps(wide)):
        o = me ^ r
        flag = (filled[o] > 0).astype(jnp.float32)
        for p in range(room // 2):
            outs[at][pl.ds(p * width, width), :] = acc[o * (room // 2) + p].astype(jnp.bfloat16)
        tail = outs[at].shape[0] - room // 2 * width
        outs[at][pl.ds(room // 2 * width, tail), :] = jnp.full(
            (tail, columns), flag, jnp.float32
        ).astype(jnp.bfloat16)


def last_kernel(wide, *refs):
    ins, out, flags = refs[: 2 * wide], refs[2 * wide], refs[2 * wide + 1]
    boxes, width, columns = out.shape
    room = 2 * boxes // wide
    me = lax.axis_index("wide")
    for at, r in enumerate(steps(wide)):
        mark = ins[at][pl.ds(room // 2 * width, 16), :].astype(jnp.float32)
        flags[me ^ r] = (jnp.max(mark) > 0.5).astype(jnp.int32)
    left = left_half((width, columns))
    for at, r in enumerate(steps(wide)):
        origin = me ^ r
        base = jnp.int32(0)
        for w in range(wide):
            base = base + jnp.where(w < origin, flags[w], 0) * room

        @pl.when(flags[origin] > 0)
        def _(at=at, base=base):
            for p in range(room // 2):
                a = ins[at][pl.ds(p * width, width), :]
                b = ins[wide + at][pl.ds(p * width, width), :]
                out[base + 2 * p] = jnp.where(left, a, swap(b))
                out[base + 2 * p + 1] = jnp.where(left, swap(a), b)


def exchange(parts, axis, size, order):
    moved = []
    for r, part in zip(order, parts):
        moved.append(lax.ppermute(part, axis, [(i, i ^ r) for i in range(size)]) if r else part)
    return moved


def cost(pair_count, width, columns, moved):
    return pl.CostEstimate(
        flops=2 * pair_count * width * width * columns, bytes_accessed=moved, transcendentals=0
    )


def per_device(
    narrow, wide, charges, pairs_first, pairs_second, pairs_third,
    matrices_first, matrices_second, matrices_third, box_owner,
):
    boxes, width, columns = charges.shape
    half = boxes // 2
    room = 2 * boxes // wide
    pair_count = pairs_first.shape[0]
    pairs_first, pairs_second, pairs_third = [
        pltpu.with_memory_space_constraint(x.T, pltpu.HBM)
        for x in (pairs_first, pairs_second, pairs_third)
    ]
    owners = pltpu.with_memory_space_constraint(box_owner.reshape(1, boxes), pltpu.HBM)
    estimate = cost(pair_count, width, columns, 4 * boxes * width * columns)

    def blocks(shape, count):
        return [jax.ShapeDtypeStruct(shape, jnp.bfloat16)] * count

    far = narrow - 2
    sent = pl.pallas_call(
        functools.partial(first_kernel, narrow),
        out_shape=blocks((half, width // narrow, columns), 2 * far)
        + blocks((2 * half, width // narrow, columns), narrow - far),
        in_specs=[HBM] * 3,
        out_specs=[VMEM] * (narrow + far),
        scratch_shapes=[
            pltpu.VMEM((boxes + 1, width, columns), jnp.float32),
            pltpu.SMEM(pairs_first.shape, jnp.int32),
            pltpu.VMEM(charges.shape, charges.dtype),
            pltpu.VMEM(matrices_first.shape, matrices_first.dtype),
            pltpu.SemaphoreType.DMA((3, PARTS)),
        ],
        cost_estimate=estimate,
        compiler_params=GRANT,
        name="first_level",
    )(*[pltpu.with_memory_space_constraint(x, pltpu.HBM) for x in (pairs_first, charges, matrices_first)])

    view = pltpu.VMEM((2 * boxes, width, columns), jnp.bfloat16)
    listed = [pltpu.SMEM(pairs_first.shape, jnp.int32), pltpu.SemaphoreType.DMA((2, 1))]
    second = lambda chunk: pl.pallas_call(
        functools.partial(second_kernel, narrow, wide, chunk),
        out_shape=blocks((half, width // wide, columns), wide),
        in_specs=[HBM, VMEM] + [VMEM] * narrow,
        out_specs=[VMEM] * wide,
        scratch_shapes=[pltpu.VMEM((half + 1, width, columns), jnp.float32), view, *listed],
        cost_estimate=estimate,
        compiler_params=GRANT,
        name="second_level",
    )
    third = pl.pallas_call(
        functools.partial(third_kernel, wide),
        out_shape=blocks((room // 2 * width + 16, columns), wide),
        in_specs=[HBM, HBM, VMEM] + [VMEM] * wide,
        out_specs=[VMEM] * wide,
        scratch_shapes=[
            pltpu.VMEM((wide * room // 2 + 1, width, columns), jnp.float32), view,
            pltpu.SMEM((wide,), jnp.int32), pltpu.SMEM((boxes,), jnp.int32),
            pltpu.SMEM((1, boxes), jnp.int32), *listed,
        ],
        cost_estimate=estimate,
        compiler_params=GRANT,
        name="third_level",
    )
    order = steps(narrow)
    first_far = exchange(sent[:far], "narrow", narrow, order[:far])
    near = exchange(sent[2 * far :], "narrow", narrow, order[far:])
    second_far = exchange(sent[far : 2 * far], "narrow", narrow, order[:far])
    moved = [
        exchange(
            second(chunk)(pairs_second, matrices_second, *parts, *near),
            "wide", wide, steps(wide),
        )
        for chunk, parts in enumerate((first_far, second_far))
    ]
    moved = [
        exchange(
            third(owners, pairs_third, matrices_third, *parts),
            "wide", wide, steps(wide),
        )
        for parts in moved
    ]
    return pl.pallas_call(
        functools.partial(last_kernel, wide),
        out_shape=jax.ShapeDtypeStruct((boxes, width, columns), jnp.bfloat16),
        in_specs=[VMEM] * (2 * wide),
        out_specs=VMEM,
        scratch_shapes=[pltpu.SMEM((wide,), jnp.int32)],
        compiler_params=GRANT,
        name="place",
    )(*moved[0], *moved[1])


def solution(mesh):
    narrow, wide = mesh.shape["narrow"], mesh.shape["wide"]
    rows = P(("wide", "narrow"), None)
    blocks = P(("wide", "narrow"), None, None)

    def body(*arrays):
        return per_device(narrow, wide, *arrays)

    return jax.shard_map(
        body,
        mesh=mesh,
        in_specs=(blocks, rows, rows, rows, blocks, blocks, blocks, P("wide", "narrow", None)),
        out_specs=blocks,
        check_vma=False,
    )
```

```python
import functools

import jax
import jax.numpy as jnp
from jax import lax
from jax.experimental import pallas as pl
from jax.experimental.pallas import tpu as pltpu
from jax.sharding import PartitionSpec as P


UNROLL = 16
PARTS = 4
GRANT = pltpu.CompilerParams(vmem_limit_bytes=16 * 2**20)
VMEM = pl.BlockSpec(memory_space=pltpu.VMEM)
SMEM = pl.BlockSpec(memory_space=pltpu.SMEM)
HBM = pl.BlockSpec(memory_space=pltpu.HBM)


def steps(size):
    top = size // 2
    far, near = list(range(top, size)), list(range(2, top))
    return far[: top // 2] + near + far[top // 2 :] + list(range(1, min(2, top))) + [0]


def left_half(shape):
    return lax.broadcasted_iota(jnp.int32, shape, len(shape) - 1) < shape[-1] // 2


def swap(block):
    return pltpu.roll(block, block.shape[-1] // 2, block.ndim - 1)


def live_count(pairs):
    count = pairs[3, 0]
    for row in range(1, pairs.shape[1]):
        count = count + pairs[3, row]
    return count


def accumulate(pairs, mats, source, place, acc):
    dummy = acc.shape[0] - 1

    def group(index, carry):
        products = []
        for step in range(UNROLL):
            row = index * UNROLL + step
            slot, half = place(pairs[1, row])
            slot = jnp.where(pairs[3, row] > 0, slot, dummy)
            product = jnp.dot(
                mats[pairs[2, row]], source(pairs[0, row], half),
                preferred_element_type=jnp.float32,
            )
            products.append((slot, product))
        for slot, product in products:
            acc[slot] += product
        return carry

    lax.fori_loop(0, (live_count(pairs) + UNROLL - 1) // UNROLL, group, 0)


def clear(acc):
    def one(index, carry):
        acc[index] = jnp.zeros(acc.shape[1:], acc.dtype)
        return carry

    lax.fori_loop(0, acc.shape[0], one, 0)


def fetch(source, target, sems, parts):
    size = source.shape[0] // parts
    copies = [
        pltpu.make_async_copy(
            source.at[pl.ds(p * size, size)], target.at[pl.ds(p * size, size)], sems.at[p]
        )
        for p in range(parts)
    ]
    for copy in copies:
        copy.start()

    def wait():
        for copy in copies:
            copy.wait()

    return wait


def first_kernel(size, pairs_hbm, charges_hbm, mats_hbm, *refs):
    count = 2 * size - 2
    outs, (acc, pairs, charges, mats, sems) = refs[:count], refs[count:]
    waits = [
        fetch(pairs_hbm, pairs, sems.at[0], 1),
        fetch(charges_hbm, charges, sems.at[1], PARTS),
        fetch(mats_hbm, mats, sems.at[2], PARTS),
    ]
    me = lax.axis_index("narrow")
    boxes, width, columns = charges.shape
    piece = width // size
    clear(acc)
    for wait in waits:
        wait()
    accumulate(
        pairs, mats, lambda s, half: charges[s], lambda k: (k, 0), acc
    )
    left = left_half((piece, columns))
    half, far = boxes // 2, size - 2
    for at, r in enumerate(steps(size)):
        rows = pl.ds(pl.multiple_of((me ^ r) * piece, piece), piece)
        targets = (outs[at], outs[far + at]) if at < far else (
            outs[far + at].at[pl.ds(0, half)], outs[far + at].at[pl.ds(half, half)]
        )

        def one(i, carry, targets=targets, rows=rows):
            a = acc[2 * i, rows, :]
            b = acc[2 * i + 1, rows, :]
            targets[0][i] = jnp.where(left, a, swap(b)).astype(jnp.bfloat16)
            targets[1][i] = jnp.where(left, swap(a), b).astype(jnp.bfloat16)
            return carry

        lax.fori_loop(0, half, one, 0, unroll=True)


def assemble(me, ins, view):
    count, piece, columns = ins[0].shape
    left = left_half((piece, columns))
    nothing = jnp.zeros((piece, columns), jnp.bfloat16)
    for r, ref in zip(steps(len(ins)), ins):
        rows = pl.ds(pl.multiple_of((me ^ r) * piece, piece), piece)
        for i in range(count):
            block = ref[i]
            turned = swap(block)
            view[4 * i, rows, :] = jnp.where(left, block, nothing)
            view[4 * i + 1, rows, :] = jnp.where(left, nothing, turned)
            view[4 * i + 2, rows, :] = jnp.where(left, turned, nothing)
            view[4 * i + 3, rows, :] = jnp.where(left, nothing, block)


def second_kernel(narrow, wide, chunk, pairs_hbm, mats, *refs):
    ins, outs = refs[:narrow], refs[narrow : narrow + wide]
    count = outs[0].shape[0]
    ins = [*ins[:-2], *(near.at[pl.ds(chunk * count, count)] for near in ins[-2:])]
    acc, view, pairs, sems = refs[narrow + wide :]
    wait = fetch(pairs_hbm, pairs, sems.at[0], 1)
    me = lax.axis_index("wide")
    count, piece, _ = outs[0].shape
    assemble(lax.axis_index("narrow"), ins, view)
    clear(acc)
    wait()
    accumulate(
        pairs, mats, lambda s, half: view[2 * s + half],
        lambda k: (k >> 1, k & 1), acc,
    )
    for at, r in enumerate(steps(wide)):
        rows = pl.ds(pl.multiple_of((me ^ r) * piece, piece), piece)
        for i in range(count):
            outs[at][i] = acc[i, rows, :].astype(jnp.bfloat16)


def third_kernel(wide, owners_hbm, pairs_hbm, mats, *refs):
    ins, outs = refs[:wide], refs[wide : 2 * wide]
    acc, view, filled, spots, owners, pairs, sems = refs[2 * wide :]
    wait = fetch(pairs_hbm, pairs, sems.at[0], 1)
    wait_owners = fetch(owners_hbm, owners, sems.at[1], 1)
    boxes = owners.shape[1]
    width, columns = acc.shape[1:]
    room = 2 * boxes // wide
    me = lax.axis_index("wide")
    assemble(me, ins, view)
    clear(acc)
    wait_owners()
    for o in range(wide):
        filled[o] = 0
    for k in range(boxes):
        o = owners[0, k]
        spots[k] = o * room + filled[o]
        filled[o] = filled[o] + 1
    wait()
    accumulate(
        pairs, mats, lambda s, half: view[2 * s + half],
        lambda k: (spots[k] >> 1, spots[k] & 1), acc,
    )
    for at, r in enumerate(steps(wide)):
        o = me ^ r
        flag = (filled[o] > 0).astype(jnp.float32)
        for p in range(room // 2):
            outs[at][pl.ds(p * width, width), :] = acc[o * (room // 2) + p].astype(jnp.bfloat16)
        tail = outs[at].shape[0] - room // 2 * width
        outs[at][pl.ds(room // 2 * width, tail), :] = jnp.full(
            (tail, columns), flag, jnp.float32
        ).astype(jnp.bfloat16)


def place_kernel(wide, chosen, *refs):
    count = len(chosen)
    firsts, seconds = refs[:wide], refs[wide : wide + count]
    out, stage, flags, sems = refs[-4:]
    boxes, width, columns = out.shape
    room = 2 * boxes // wide
    me = lax.axis_index("wide")
    order = steps(wide)
    for at, r in enumerate(order):
        mark = firsts[at][pl.ds(room // 2 * width, 16), :].astype(jnp.float32)
        flags[me ^ r] = (jnp.max(mark) > 0.5).astype(jnp.int32)
    left = left_half((width, columns))
    moves = []
    for at, r in enumerate(chosen):
        origin = me ^ r
        base = jnp.int32(0)
        for w in range(wide):
            base = base + jnp.where(w < origin, flags[w], 0) * room
        copies = [
            pltpu.make_async_copy(
                stage.at[pl.ds(base + 2 * p, 2)], out.at[pl.ds(base + 2 * p, 2)], sems.at[at, p]
            )
            for p in range(room // 2)
        ]
        moves.append((origin, copies))

        @pl.when(flags[origin] > 0)
        def _(a_ref=firsts[order.index(r)], b_ref=seconds[at], base=base, copies=copies):
            for p, copy in enumerate(copies):
                a = a_ref[pl.ds(p * width, width), :]
                b = b_ref[pl.ds(p * width, width), :]
                stage[base + 2 * p] = jnp.where(left, a, swap(b))
                stage[base + 2 * p + 1] = jnp.where(left, swap(a), b)
                copy.start()

    for origin, copies in moves:

        @pl.when(flags[origin] > 0)
        def _(copies=copies):
            for copy in copies:
                copy.wait()


def exchange(parts, axis, size, order):
    moved = []
    for r, part in zip(order, parts):
        moved.append(lax.ppermute(part, axis, [(i, i ^ r) for i in range(size)]) if r else part)
    return moved


def cost(pair_count, width, columns, moved):
    return pl.CostEstimate(
        flops=2 * pair_count * width * width * columns, bytes_accessed=moved, transcendentals=0
    )


def per_device(
    narrow, wide, charges, pairs_first, pairs_second, pairs_third,
    matrices_first, matrices_second, matrices_third, box_owner,
):
    boxes, width, columns = charges.shape
    half = boxes // 2
    room = 2 * boxes // wide
    pair_count = pairs_first.shape[0]
    pairs_first, pairs_second, pairs_third = [
        pltpu.with_memory_space_constraint(x.T, pltpu.HBM)
        for x in (pairs_first, pairs_second, pairs_third)
    ]
    owners = pltpu.with_memory_space_constraint(box_owner.reshape(1, boxes), pltpu.HBM)
    estimate = cost(pair_count, width, columns, 4 * boxes * width * columns)

    def blocks(shape, count):
        return [jax.ShapeDtypeStruct(shape, jnp.bfloat16)] * count

    far = narrow - 2
    sent = pl.pallas_call(
        functools.partial(first_kernel, narrow),
        out_shape=blocks((half, width // narrow, columns), 2 * far)
        + blocks((2 * half, width // narrow, columns), narrow - far),
        in_specs=[HBM] * 3,
        out_specs=[VMEM] * (narrow + far),
        scratch_shapes=[
            pltpu.VMEM((boxes + 1, width, columns), jnp.float32),
            pltpu.SMEM(pairs_first.shape, jnp.int32),
            pltpu.VMEM(charges.shape, charges.dtype),
            pltpu.VMEM(matrices_first.shape, matrices_first.dtype),
            pltpu.SemaphoreType.DMA((3, PARTS)),
        ],
        cost_estimate=estimate,
        compiler_params=GRANT,
        name="first_level",
    )(*[pltpu.with_memory_space_constraint(x, pltpu.HBM) for x in (pairs_first, charges, matrices_first)])

    view = pltpu.VMEM((2 * boxes, width, columns), jnp.bfloat16)
    listed = [pltpu.SMEM(pairs_first.shape, jnp.int32), pltpu.SemaphoreType.DMA((2, 1))]
    second = lambda chunk: pl.pallas_call(
        functools.partial(second_kernel, narrow, wide, chunk),
        out_shape=blocks((half, width // wide, columns), wide),
        in_specs=[HBM, VMEM] + [VMEM] * narrow,
        out_specs=[VMEM] * wide,
        scratch_shapes=[pltpu.VMEM((half + 1, width, columns), jnp.float32), view, *listed],
        cost_estimate=estimate,
        compiler_params=GRANT,
        name="second_level",
    )
    third = pl.pallas_call(
        functools.partial(third_kernel, wide),
        out_shape=blocks((room // 2 * width + 16, columns), wide),
        in_specs=[HBM, HBM, VMEM] + [VMEM] * wide,
        out_specs=[VMEM] * wide,
        scratch_shapes=[
            pltpu.VMEM((wide * room // 2 + 1, width, columns), jnp.float32), view,
            pltpu.SMEM((wide,), jnp.int32), pltpu.SMEM((boxes,), jnp.int32),
            pltpu.SMEM((1, boxes), jnp.int32), *listed,
        ],
        cost_estimate=estimate,
        compiler_params=GRANT,
        name="third_level",
    )
    order = steps(narrow)
    first_far = exchange(sent[:far], "narrow", narrow, order[:far])
    near = exchange(sent[2 * far :], "narrow", narrow, order[far:])
    second_far = exchange(sent[far : 2 * far], "narrow", narrow, order[:far])
    moved = [
        exchange(
            second(chunk)(pairs_second, matrices_second, *parts, *near),
            "wide", wide, steps(wide),
        )
        for chunk, parts in enumerate((first_far, second_far))
    ]
    moved = [
        exchange(
            third(owners, pairs_third, matrices_third, *parts),
            "wide", wide, steps(wide),
        )
        for parts in moved
    ]
    firsts, seconds = moved
    late = steps(wide).index(1)
    early = [r for r in steps(wide) if r != 1]

    def place(chosen, parts, start=()):
        return pl.pallas_call(
            functools.partial(place_kernel, wide, chosen),
            out_shape=jax.ShapeDtypeStruct((boxes, width, columns), jnp.bfloat16),
            in_specs=[VMEM] * (wide + len(parts)) + [HBM] * len(start),
            out_specs=HBM,
            input_output_aliases={wide + len(parts): 0} if start else {},
            scratch_shapes=[
                pltpu.VMEM((boxes, width, columns), jnp.bfloat16),
                pltpu.SMEM((wide,), jnp.int32),
                pltpu.SemaphoreType.DMA((len(chosen), room // 2)),
            ],
            compiler_params=GRANT,
        )(*firsts, *parts, *start)

    begun = place(early, seconds[:late] + seconds[late + 1 :])
    return place([1], [seconds[late]], [begun])


def solution(mesh):
    narrow, wide = mesh.shape["narrow"], mesh.shape["wide"]
    rows = P(("wide", "narrow"), None)
    blocks = P(("wide", "narrow"), None, None)

    def body(*arrays):
        return per_device(narrow, wide, *arrays)

    return jax.shard_map(
        body,
        mesh=mesh,
        in_specs=(blocks, rows, rows, rows, blocks, blocks, blocks, P("wide", "narrow", None)),
        out_specs=blocks,
        check_vma=False,
    )
```
